32 devices in a mesh: model: 8 (over z, y), data: 4 (over x, core).
Axes of the slice: x: 2, y: 2, z: 4, core: 2. Of those that a mesh axis runs over, the one named last changes fastest.
Arguments:
- local_grads: bfloat16 [4, 144, 262144], P('data', None, 'model')
- master: float32 [144, 262144], P(None, ('model', 'data'))
- moment_one: float32 [144, 262144], P(None, ('model', 'data'))
- moment_two: float32 [144, 262144], P(None, ('model', 'data'))
Outputs:
- output 1: bfloat16 [144, 262144], P(None, 'model')
- output 2: float32 [144, 262144], P(None, ('model', 'data'))
- output 3: float32 [144, 262144], P(None, ('model', 'data'))
- output 4: float32 [144, 262144], P(None, ('model', 'data'))
All inputs are finite; a program needn't handle non-finite values.
Results may differ from the reference program's by a relative error of at most 0.001.
Values are sent between devices in bfloat16 or wider.
A program may use at most 1 GiB of HBM per device.

```python
import jax
import jax.numpy as jnp
from jax import lax

D = 512
LAYERS = 12
DATA = 4
STEP = 4
BLOCKS = 12 * LAYERS
BLOCK_SIZE = D * D
LEARN_RATE = 0.08
BETA_ONE = 0.9
BETA_TWO = 0.999
EPSILON = 1e-6
WEIGHT_DECAY = 0.01
MAX_NORM = 1.0
CORR_ONE = 1.0 - BETA_ONE ** STEP
CORR_TWO = 1.0 - BETA_TWO ** STEP


def tensor_sums(block_values):
    return jnp.stack([block_values[..., 0:3].sum(axis=-1), block_values[..., 3], block_values[..., 4:8].sum(axis=-1), block_values[..., 8:12].sum(axis=-1)], axis=-1)


def spread_tensors(tensor_values):
    lead_shape = tensor_values.shape[:-1]
    pieces = [jnp.broadcast_to(tensor_values[..., tensor_pos:tensor_pos + 1], lead_shape + (block_count,)) for tensor_pos, block_count in enumerate((3, 1, 4, 4))]
    return jnp.concatenate(pieces, axis=-1)


def setup_inputs(seed: int = 0) -> dict:
    key_list = jax.random.split(jax.random.key(seed), 8)
    fan_scale = jnp.concatenate([jnp.full((8,), D ** -0.5, jnp.float32), jnp.full((4,), (4 * D) ** -0.5, jnp.float32)])
    weight_factor = jnp.exp(jax.random.uniform(key_list[0], (LAYERS, 4), jnp.float32, minval=-0.8, maxval=0.8))
    weight_scale = (spread_tensors(weight_factor) * fan_scale).reshape(BLOCKS, 1)
    weight_slope = spread_tensors(jax.random.uniform(key_list[1], (LAYERS, 4), jnp.float32, minval=1.5, maxval=2.5)).reshape(BLOCKS, 1)
    position = jnp.arange(BLOCK_SIZE, dtype=jnp.float32) / BLOCK_SIZE - 0.5
    grad_factor = spread_tensors(jnp.exp(jax.random.uniform(key_list[2], (LAYERS, 4), jnp.float32, minval=-1.0, maxval=1.0))).reshape(BLOCKS, 1)
    grad_sigma = grad_factor * (3.0 * MAX_NORM) / jnp.sqrt(BLOCK_SIZE * jnp.sum(grad_factor * grad_factor))
    unit_scale = grad_sigma / jnp.sqrt(2.0)
    shared = jax.random.normal(key_list[3], (BLOCKS, BLOCK_SIZE), jnp.float32)

    def one_replica(replica):
        replica_noise = jax.random.normal(jax.random.fold_in(key_list[4], replica), (BLOCKS, BLOCK_SIZE), jnp.float32)
        return (unit_scale * (shared + DATA ** 0.5 * replica_noise)).astype(jnp.bfloat16)

    local_grads = lax.map(one_replica, jnp.arange(DATA))
    step_sigma = grad_sigma / 3.0
    master = weight_scale * jnp.exp(weight_slope * position) * jax.random.normal(key_list[5], (BLOCKS, BLOCK_SIZE), jnp.float32)
    moment_one = 0.1 * step_sigma * jax.random.normal(key_list[6], (BLOCKS, BLOCK_SIZE), jnp.float32)
    moment_two = 0.003 * step_sigma * step_sigma * jax.random.uniform(key_list[7], (BLOCKS, BLOCK_SIZE), jnp.float32, minval=0.5, maxval=1.5)
    return {'local_grads': local_grads, 'master': master, 'moment_one': moment_one, 'moment_two': moment_two}


def reference(local_grads, master, moment_one, moment_two):
    grad_mean = jnp.sum(local_grads, axis=0, dtype=jnp.float32) / DATA
    clip_scale = jnp.minimum(1.0, MAX_NORM / jnp.sqrt(jnp.sum(grad_mean * grad_mean)))
    scaled = clip_scale * grad_mean
    new_one = BETA_ONE * moment_one + (1.0 - BETA_ONE) * scaled
    new_two = BETA_TWO * moment_two + (1.0 - BETA_TWO) * scaled * scaled
    direction = (new_one / CORR_ONE) / (jnp.sqrt(new_two / CORR_TWO) + EPSILON) + WEIGHT_DECAY * master
    norm_sq = jnp.stack([jnp.sum(master * master, axis=1), jnp.sum(direction * direction, axis=1)])
    tensor_norms = jnp.sqrt(tensor_sums(norm_sq.reshape(2, LAYERS, 12)))
    block_ratio = spread_tensors(tensor_norms[0] / tensor_norms[1]).reshape(BLOCKS, 1)
    new_master = master - LEARN_RATE * block_ratio * direction
    return new_master.astype(jnp.bfloat16), new_master, new_one, new_two
```

```python
import functools

import jax
import jax.numpy as jnp
from jax import lax
from jax.experimental import pallas as pl
from jax.experimental.pallas import tpu as pltpu
from jax.sharding import PartitionSpec as P

STEP = 4
LEARN_RATE = 0.08
BETA_ONE = 0.9
BETA_TWO = 0.999
EPSILON = 1e-6
WEIGHT_DECAY = 0.01
MAX_NORM = 1.0
CORR_ONE = 1.0 - BETA_ONE ** STEP
CORR_TWO = 1.0 - BETA_TWO ** STEP

MESH = pl.DeviceIdType.MESH
LANES = 128
SUBLANES = 8
CHUNK_ROWS = 16
SUM_COLS = 512
STEP_COLS = 1024
BLOCKS_PER_LAYER = 12
TENSOR_STARTS = (0, 3, 4, 8)


def lane_fold(values):
    total = values[:, :LANES]
    for start in range(LANES, values.shape[1], LANES):
        total = total + values[:, start:start + LANES]
    return total


def tensor_mask(rows):
    row = lax.broadcasted_iota(jnp.int32, (rows, LANES), 0)
    lane = lax.broadcasted_iota(jnp.int32, (rows, LANES), 1)
    layer = row // BLOCKS_PER_LAYER
    block = row - layer * BLOCKS_PER_LAYER
    tensor = layer * len(TENSOR_STARTS)
    for start in TENSOR_STARTS[1:]:
        tensor = tensor + (block >= start).astype(jnp.int32)
    return tensor == lane


def step_kernel(model_size, data_size, grads, master, moment_one, moment_two,
                new_params, new_master, new_one, new_two,
                gathered, grad_mean, row_sq, row_scale, clip_rows, norm_rows,
                load_sem, own_sem, sum_send, sum_recv, small_send, small_recv,
                out_send, out_recv, fwd_send, fwd_recv):
    rows, width = new_master.shape
    chunks = rows // CHUNK_ROWS
    devices = model_size * data_size
    my_model = lax.axis_index('model')
    my_data = lax.axis_index('data')
    me = my_model * data_size + my_data
    partner = my_data + 1 - 2 * lax.rem(my_data, 2)
    across = lax.rem(my_data + 2, data_size)
    across_partner = lax.rem(partner + 2, data_size)
    peers = (my_data, partner, across, across_partner)

    def device_at(index):
        return (index // data_size, lax.rem(index, data_size))

    loads = [pltpu.make_async_copy(src, dst, load_sem.at[i]) for i, (src, dst) in enumerate(
        ((master, new_master), (moment_one, new_one), (moment_two, new_two)))]

    barrier = pltpu.get_barrier_semaphore()

    @pl.loop(1, devices)
    def _(offset):
        pl.semaphore_signal(barrier, inc=1, device_id=device_at(lax.rem(me + offset, devices)), device_id_type=MESH)
    pl.semaphore_wait(barrier, devices - 1)

    def grad_part(slot, chunk):
        return grads.at[0, pl.ds(chunk * CHUNK_ROWS, CHUNK_ROWS), pl.ds(pl.multiple_of(peers[slot] * width, LANES), width)]

    def slot_part(slot, chunk):
        return gathered.at[slot, pl.ds(chunk * CHUNK_ROWS, CHUNK_ROWS)]

    def own_copy(chunk):
        return pltpu.make_async_copy(grad_part(0, chunk), slot_part(0, chunk), own_sem.at[chunk])

    def grad_copy(slot, chunk):
        return pltpu.make_async_remote_copy(grad_part(slot, chunk), slot_part(slot, chunk), sum_send.at[slot], sum_recv.at[slot, chunk], device_id=(my_model, peers[slot]), device_id_type=MESH)

    @pl.loop(0, chunks)
    def _(chunk):
        for slot in (2, 3, 1):
            grad_copy(slot, chunk).start()
        own_copy(chunk).start()

    for load in loads:
        load.start()
    for load in loads:
        load.wait()

    mask = tensor_mask(rows)

    def square_rows(ref):
        @pl.loop(0, rows // SUBLANES)
        def _(group):
            row = pl.ds(pl.multiple_of(group * SUBLANES, SUBLANES), SUBLANES)

            def fold(block, total):
                part = ref[row, pl.ds(pl.multiple_of(block * STEP_COLS, LANES), STEP_COLS)]
                return total + lane_fold(part * part)
            row_sq[row, :] = lax.fori_loop(0, width // STEP_COLS, fold, jnp.zeros((SUBLANES, LANES), jnp.float32))

    def tensor_row():
        per_row = jnp.sum(row_sq[...], axis=1, keepdims=True)
        return jnp.sum(jnp.where(mask, per_row, 0.0), axis=0, keepdims=True)

    def small_copy(which, table, target):
        return pltpu.make_async_remote_copy(table.at[pl.ds(me, 1)], table.at[pl.ds(me, 1)], small_send.at[which], small_recv.at[which], device_id=device_at(target), device_id_type=MESH)

    def send_row(which, table, row):
        table[pl.ds(me, 1), :] = row

        @pl.loop(1, devices)
        def _(offset):
            small_copy(which, table, lax.rem(me + offset, devices)).start()

    def all_rows(which, table):
        rest = table.at[pl.ds(0, devices - 1)]
        pltpu.make_async_remote_copy(rest, rest, small_send.at[which], small_recv.at[which], device_id=(my_model, my_data), device_id_type=MESH).wait()
        return jnp.sum(table[...], axis=0, keepdims=True)

    square_rows(new_master)
    send_row(0, norm_rows.at[0], tensor_row())

    def add_chunk(chunk, total):
        own_copy(chunk).wait()
        for slot in (1, 2, 3):
            grad_copy(slot, chunk).wait_recv()
        row = pl.ds(pl.multiple_of(chunk * CHUNK_ROWS, CHUNK_ROWS), CHUNK_ROWS)

        def add_block(block, total):
            col = pl.ds(pl.multiple_of(block * SUM_COLS, LANES), SUM_COLS)
            part = [gathered[slot, row, col].astype(jnp.float32) for slot in range(data_size)]
            mean = ((part[0] + part[1]) + (part[2] + part[3])) * (1.0 / data_size)
            grad_mean[row, col] = mean
            return total + lane_fold(mean * mean)
        return lax.fori_loop(0, width // SUM_COLS, add_block, total)

    grad_sq = lax.fori_loop(0, chunks, add_chunk, jnp.zeros((CHUNK_ROWS, LANES), jnp.float32))
    send_row(1, clip_rows, jnp.sum(grad_sq, axis=0, keepdims=True))
    total_sq = jnp.sum(all_rows(1, clip_rows), axis=1, keepdims=True)
    clip = jnp.minimum(1.0, MAX_NORM / jnp.sqrt(total_sq))
    one_scale = jnp.broadcast_to((1.0 - BETA_ONE) * clip, (SUBLANES, STEP_COLS))
    two_scale = jnp.broadcast_to((1.0 - BETA_TWO) * clip * clip, (SUBLANES, STEP_COLS))

    @pl.loop(0, rows // SUBLANES)
    def _(group):
        row = pl.ds(pl.multiple_of(group * SUBLANES, SUBLANES), SUBLANES)

        def step_block(block, total):
            col = pl.ds(pl.multiple_of(block * STEP_COLS, LANES), STEP_COLS)
            grad = grad_mean[row, col]
            one = BETA_ONE * new_one[row, col] + one_scale * grad
            two = BETA_TWO * new_two[row, col] + two_scale * grad * grad
            new_one[row, col] = one
            new_two[row, col] = two
            direction = (one * (1.0 / CORR_ONE)) / (jnp.sqrt(two * (1.0 / CORR_TWO)) + EPSILON) + WEIGHT_DECAY * new_master[row, col]
            grad_mean[row, col] = direction
            return total + lane_fold(direction * direction)
        row_sq[row, :] = lax.fori_loop(0, width // STEP_COLS, step_block, jnp.zeros((SUBLANES, LANES), jnp.float32))

    send_row(2, norm_rows.at[1], tensor_row())
    weight_sq = all_rows(0, norm_rows.at[0])
    step_sq = all_rows(2, norm_rows.at[1])
    ratio = LEARN_RATE * (jnp.sqrt(weight_sq) / jnp.sqrt(step_sq))
    scale = jnp.sum(jnp.where(mask, ratio, 0.0), axis=1, keepdims=True)
    row_scale[...] = jnp.broadcast_to(scale, (rows, LANES))

    my_col = pl.multiple_of(my_data * width, LANES)

    def update_chunk(chunk):
        row = pl.ds(pl.multiple_of(chunk * CHUNK_ROWS, CHUNK_ROWS), CHUNK_ROWS)
        rate = jnp.broadcast_to(row_scale[row, 0:1], (CHUNK_ROWS, SUM_COLS))

        @pl.loop(0, width // SUM_COLS)
        def _(block):
            start = pl.multiple_of(block * SUM_COLS, LANES)
            col = pl.ds(start, SUM_COLS)
            updated = new_master[row, col] - rate * grad_mean[row, col]
            new_master[row, col] = updated
            new_params[row, pl.ds(pl.multiple_of(my_col + start, LANES), SUM_COLS)] = updated.astype(jnp.bfloat16)

    def params_part(owner, chunk):
        return new_params.at[pl.ds(chunk * CHUNK_ROWS, CHUNK_ROWS), pl.ds(pl.multiple_of(owner * width, LANES), width)]

    def params_copy(owner, target, chunk, send, recv):
        part = params_part(owner, chunk)
        return pltpu.make_async_remote_copy(part, part, send, recv, device_id=(my_model, target), device_id_type=MESH)

    def across_copy(chunk):
        return params_copy(my_data, across, chunk, out_send.at[0], out_recv.at[0, chunk])

    def partner_copy(chunk):
        return params_copy(my_data, partner, chunk, out_send.at[1], out_recv.at[1, chunk])

    def forward_copy(chunk):
        return params_copy(across, partner, chunk, fwd_send.at[0], fwd_recv.at[chunk])

    update_chunk(0)

    @pl.loop(1, chunks)
    def _(chunk):
        update_chunk(chunk)
        across_copy(chunk - 1).start()
        partner_copy(chunk - 1).start()
    across_copy(chunks - 1).start()
    partner_copy(chunks - 1).start()

    @pl.loop(0, chunks)
    def _(chunk):
        across_copy(chunk).wait_recv()
        forward_copy(chunk).start()

    @pl.loop(0, chunks)
    def _(chunk):
        partner_copy(chunk).wait_recv()
        forward_copy(chunk).wait_recv()

    whole = new_params.at[:, pl.ds(0, width)]
    for send in (out_send.at[0], out_send.at[1], fwd_send.at[0]):
        pltpu.make_async_remote_copy(whole, whole, send, out_recv.at[0, 0], device_id=(my_model, partner), device_id_type=MESH).wait_send()
    for slot in (1, 2, 3):
        pltpu.make_async_remote_copy(gathered.at[0], gathered.at[0], sum_send.at[slot], out_recv.at[0, 0], device_id=(my_model, partner), device_id_type=MESH).wait_send()


def write_kernel(count, *refs):
    sources, targets, sems = refs[:count], refs[count:2 * count], refs[2 * count]
    copies = [pltpu.make_async_copy(src, dst, sems.at[i]) for i, (src, dst) in enumerate(zip(sources, targets))]
    for copy in copies:
        copy.start()
    for copy in copies:
        copy.wait()


def solution(mesh):
    model_size, data_size = mesh.shape['model'], mesh.shape['data']
    devices = model_size * data_size
    state_spec = P(None, ('model', 'data'))

    def device_step(local_grads, master, moment_one, moment_two):
        rows, width = master.shape
        chunks = rows // CHUNK_ROWS
        hbm = pl.BlockSpec(memory_space=pltpu.HBM)
        vmem = pl.BlockSpec(memory_space=pltpu.VMEM)
        state = pltpu.VMEM((rows, width), jnp.float32)
        held = pl.pallas_call(
            functools.partial(step_kernel, model_size, data_size),
            out_shape=(pltpu.VMEM((rows, width * data_size), jnp.bfloat16), state, state, state),
            in_specs=[hbm] * 4,
            out_specs=[vmem] * 4,
            scratch_shapes=[
                pltpu.VMEM((data_size, rows, width), jnp.bfloat16),
                pltpu.VMEM((rows, width), jnp.float32),
                pltpu.VMEM((rows, LANES), jnp.float32),
                pltpu.VMEM((rows, LANES), jnp.float32),
                pltpu.VMEM((devices, LANES), jnp.float32),
                pltpu.VMEM((2, devices, LANES), jnp.float32),
                pltpu.SemaphoreType.DMA((3,)),
                pltpu.SemaphoreType.DMA((chunks,)),
                pltpu.SemaphoreType.DMA((data_size,)),
                pltpu.SemaphoreType.DMA((data_size, chunks)),
                pltpu.SemaphoreType.DMA((3,)),
                pltpu.SemaphoreType.DMA((3,)),
                pltpu.SemaphoreType.DMA((2,)),
                pltpu.SemaphoreType.DMA((2, chunks)),
                pltpu.SemaphoreType.DMA((1,)),
                pltpu.SemaphoreType.DMA((chunks,)),
            ],
            compiler_params=pltpu.CompilerParams(collective_id=0, has_side_effects=True, vmem_limit_bytes=38 * 2 ** 20),
            name='lamb_step',
        )(local_grads, master, moment_one, moment_two)
        return pl.pallas_call(
            functools.partial(write_kernel, len(held)),
            out_shape=tuple(jax.ShapeDtypeStruct(a.shape, a.dtype) for a in held),
            in_specs=[vmem] * len(held),
            out_specs=[hbm] * len(held),
            scratch_shapes=[pltpu.SemaphoreType.DMA((len(held),))],
            compiler_params=pltpu.CompilerParams(vmem_limit_bytes=2 ** 20),
            name='write_out',
        )(*held)

    return jax.shard_map(device_step, mesh=mesh, in_specs=(P('data', None, 'model'), state_spec, state_spec, state_spec), out_specs=(P(None, 'model'), state_spec, state_spec, state_spec), check_vma=False)
```

```python
import functools

import jax
import jax.numpy as jnp
from jax import lax
from jax.experimental import pallas as pl
from jax.experimental.pallas import tpu as pltpu
from jax.sharding import PartitionSpec as P

STEP = 4
LEARN_RATE = 0.08
BETA_ONE = 0.9
BETA_TWO = 0.999
EPSILON = 1e-6
WEIGHT_DECAY = 0.01
MAX_NORM = 1.0
CORR_ONE = 1.0 - BETA_ONE ** STEP
CORR_TWO = 1.0 - BETA_TWO ** STEP


MESH = pl.DeviceIdType.MESH
LANES = 128
SUBLANES = 8
CHUNK_ROWS = 16
SUM_COLS = 512
STEP_COLS = 1024
BLOCKS_PER_LAYER = 12
TENSOR_STARTS = (0, 3, 4, 8)
GROUP_ROWS = (0, 16, 64, 144)
EARLY_ROWS = 128
PLANE = 2
LEVELS = 4
WRITE_BYTES = 2 ** 20


def lane_fold(values):
    total = values[:, :LANES]
    for start in range(LANES, values.shape[1], LANES):
        total = total + values[:, start:start + LANES]
    return total


def tensor_mask(first, last):
    row = first + lax.broadcasted_iota(jnp.int32, (last - first, LANES), 0)
    lane = lax.broadcasted_iota(jnp.int32, (last - first, LANES), 1)
    layer = row // BLOCKS_PER_LAYER
    block = row - layer * BLOCKS_PER_LAYER
    tensor = layer * len(TENSOR_STARTS)
    for start in TENSOR_STARTS[1:]:
        tensor = tensor + (block >= start).astype(jnp.int32)
    return tensor == lane


def step_kernel(model_size, data_size, grads, master, moment_one, moment_two,
                new_params, new_master, new_one, new_two,
                gathered, grad_mean, row_sq, row_scale, clip_rows, norm_rows,
                load_sem, level_sem, own_sem, sum_send, sum_recv, small_send, small_recv,
                out_send, out_recv, fwd_send, fwd_recv):
    rows, width = new_master.shape
    chunks = rows // CHUNK_ROWS
    devices = model_size * data_size
    my_model = lax.axis_index('model')
    my_data = lax.axis_index('data')
    me = my_model * data_size + my_data
    partner = my_data + 1 - 2 * lax.rem(my_data, 2)
    across = lax.rem(my_data + 2, data_size)
    across_partner = lax.rem(partner + 2, data_size)
    peers = (my_data, partner, across, across_partner)

    def device_at(index):
        return (index // data_size, lax.rem(index, data_size))

    loads = [pltpu.make_async_copy(src, dst, load_sem.at[i]) for i, (src, dst) in enumerate(
        ((master, new_master), (moment_one, new_one), (moment_two, new_two)))]

    plane = my_model // PLANE
    planes = model_size // PLANE
    in_plane = my_model - plane * PLANE
    degree = data_size + jnp.minimum(plane, 1) + jnp.minimum(planes - 1 - plane, 1)

    def tell_neighbours(sem):
        for target in ((my_model, partner), (my_model, across), (my_model, across_partner), (plane * PLANE + PLANE - 1 - in_plane, my_data)):
            pl.semaphore_signal(sem, inc=1, device_id=target, device_id_type=MESH)

        @pl.when(plane > 0)
        def _():
            pl.semaphore_signal(sem, inc=1, device_id=(my_model - PLANE, my_data), device_id_type=MESH)

        @pl.when(plane < planes - 1)
        def _():
            pl.semaphore_signal(sem, inc=1, device_id=(my_model + PLANE, my_data), device_id_type=MESH)

    with jax.named_scope('entry'):
        barrier = pltpu.get_barrier_semaphore()
        tell_neighbours(barrier)
        pl.semaphore_wait(barrier, degree)

    def grad_part(slot, chunk):
        return grads.at[0, pl.ds(chunk * CHUNK_ROWS, CHUNK_ROWS), pl.ds(pl.multiple_of(peers[slot] * width, LANES), width)]

    def slot_part(slot, chunk):
        return gathered.at[slot, pl.ds(chunk * CHUNK_ROWS, CHUNK_ROWS)]

    def own_copy(chunk):
        return pltpu.make_async_copy(grad_part(0, chunk), slot_part(0, chunk), own_sem.at[chunk])

    def grad_copy(slot, chunk):
        return pltpu.make_async_remote_copy(grad_part(slot, chunk), slot_part(slot, chunk), sum_send.at[slot], sum_recv.at[slot, chunk], device_id=(my_model, peers[slot]), device_id_type=MESH)

    with jax.named_scope('issue'):
        @pl.loop(0, chunks)
        def _(chunk):
            for slot in (2, 3, 1):
                grad_copy(slot, chunk).start()
            own_copy(chunk).start()

        for load in loads:
            load.start()
    with jax.named_scope('levels'):
        for level in range(LEVELS):
            tell_neighbours(level_sem.at[level])
            pl.semaphore_wait(level_sem.at[level], degree)

    with jax.named_scope('loadwait'):
        for load in loads:
            load.wait()

    def square_rows(ref):
        @pl.loop(0, rows // SUBLANES)
        def _(group):
            row = pl.ds(pl.multiple_of(group * SUBLANES, SUBLANES), SUBLANES)

            def fold(block, total):
                part = ref[row, pl.ds(pl.multiple_of(block * STEP_COLS, LANES), STEP_COLS)]
                return total + lane_fold(part * part)
            row_sq[row, :] = lax.fori_loop(0, width // STEP_COLS, fold, jnp.zeros((SUBLANES, LANES), jnp.float32))

    def tensor_row(first, last):
        per_row = jnp.sum(row_sq[first:last, :], axis=1, keepdims=True)
        return jnp.sum(jnp.where(tensor_mask(first, last), per_row, 0.0), axis=0, keepdims=True)

    def small_copy(which, table, target):
        return pltpu.make_async_remote_copy(table.at[pl.ds(me, 1)], table.at[pl.ds(me, 1)], small_send.at[which], small_recv.at[which], device_id=device_at(target), device_id_type=MESH)

    def send_row(which, table, row):
        table[pl.ds(me, 1), :] = row

        @pl.loop(1, devices)
        def _(offset):
            small_copy(which, table, lax.rem(me + offset, devices)).start()

    def all_rows(which, table):
        rest = table.at[pl.ds(0, devices - 1)]
        pltpu.make_async_remote_copy(rest, rest, small_send.at[which], small_recv.at[which], device_id=(my_model, my_data), device_id_type=MESH).wait()
        return jnp.sum(table[...], axis=0, keepdims=True)

    with jax.named_scope('wsq'):
        square_rows(new_master)
        send_row(0, norm_rows.at[0], tensor_row(0, rows))

    def add_chunk(chunk, total):
        own_copy(chunk).wait()
        for slot in (1, 2, 3):
            grad_copy(slot, chunk).wait_recv()
        row = pl.ds(pl.multiple_of(chunk * CHUNK_ROWS, CHUNK_ROWS), CHUNK_ROWS)

        def add_block(block, total):
            col = pl.ds(pl.multiple_of(block * SUM_COLS, LANES), SUM_COLS)
            part = [gathered[slot, row, col].astype(jnp.float32) for slot in range(data_size)]
            mean = ((part[0] + part[1]) + (part[2] + part[3])) * (1.0 / data_size)
            grad_mean[row, col] = mean
            return total + lane_fold(mean * mean)
        return lax.fori_loop(0, width // SUM_COLS, add_block, total)

    with jax.named_scope('wnorm'):
        rate_norm = LEARN_RATE * jnp.sqrt(all_rows(0, norm_rows.at[0]))
    with jax.named_scope('sumgrad'):
        grad_sq = lax.fori_loop(0, chunks, add_chunk, jnp.zeros((CHUNK_ROWS, LANES), jnp.float32))
    with jax.named_scope('ar_n'):
        send_row(1, clip_rows, jnp.sum(grad_sq, axis=0, keepdims=True))
        total_sq = jnp.sum(all_rows(1, clip_rows), axis=1, keepdims=True)
    clip = jnp.minimum(1.0, MAX_NORM / jnp.sqrt(total_sq))
    one_scale = jnp.broadcast_to((1.0 - BETA_ONE) * clip, (SUBLANES, STEP_COLS))
    two_scale = jnp.broadcast_to((1.0 - BETA_TWO) * clip * clip, (SUBLANES, STEP_COLS))

    def moments(first, last):
        @pl.loop(first // SUBLANES, last // SUBLANES)
        def _(group):
            row = pl.ds(pl.multiple_of(group * SUBLANES, SUBLANES), SUBLANES)

            def step_block(block, total):
                col = pl.ds(pl.multiple_of(block * STEP_COLS, LANES), STEP_COLS)
                grad = grad_mean[row, col]
                one = BETA_ONE * new_one[row, col] + one_scale * grad
                two = BETA_TWO * new_two[row, col] + two_scale * grad * grad
                new_one[row, col] = one
                new_two[row, col] = two
                direction = (one * (1.0 / CORR_ONE)) / (jnp.sqrt(two * (1.0 / CORR_TWO)) + EPSILON) + WEIGHT_DECAY * new_master[row, col]
                grad_mean[row, col] = direction
                return total + lane_fold(direction * direction)
            row_sq[row, :] = lax.fori_loop(0, width // STEP_COLS, step_block, jnp.zeros((SUBLANES, LANES), jnp.float32))

    my_col = pl.multiple_of(my_data * width, LANES)

    def update_chunk(chunk):
        row = pl.ds(pl.multiple_of(chunk * CHUNK_ROWS, CHUNK_ROWS), CHUNK_ROWS)
        rate = jnp.broadcast_to(row_scale[row, 0:1], (CHUNK_ROWS, SUM_COLS))

        @pl.loop(0, width // SUM_COLS)
        def _(block):
            start = pl.multiple_of(block * SUM_COLS, LANES)
            col = pl.ds(start, SUM_COLS)
            updated = new_master[row, col] - rate * grad_mean[row, col]
            new_master[row, col] = updated
            new_params[row, pl.ds(pl.multiple_of(my_col + start, LANES), SUM_COLS)] = updated.astype(jnp.bfloat16)

    def params_part(owner, chunk):
        return new_params.at[pl.ds(chunk * CHUNK_ROWS, CHUNK_ROWS), pl.ds(pl.multiple_of(owner * width, LANES), width)]

    def params_copy(owner, target, chunk, send, recv):
        part = params_part(owner, chunk)
        return pltpu.make_async_remote_copy(part, part, send, recv, device_id=(my_model, target), device_id_type=MESH)

    def across_copy(chunk):
        return params_copy(my_data, across, chunk, out_send.at[0], out_recv.at[0, chunk])

    def partner_copy(chunk):
        return params_copy(my_data, partner, chunk, out_send.at[1], out_recv.at[1, chunk])

    def forward_copy(chunk):
        return params_copy(across, partner, chunk, fwd_send.at[0], fwd_recv.at[chunk])

    def share(index):
        send_row(2 + index, norm_rows.at[1 + index], tensor_row(GROUP_ROWS[index], GROUP_ROWS[index + 1]))

    def finish(index):
        first, last = GROUP_ROWS[index], GROUP_ROWS[index + 1]
        ratio = rate_norm / jnp.sqrt(all_rows(2 + index, norm_rows.at[1 + index]))
        scale = jnp.sum(jnp.where(tensor_mask(first, last), ratio, 0.0), axis=1, keepdims=True)
        row_scale[first:last, :] = jnp.broadcast_to(scale, (last - first, LANES))

        @pl.loop(first // CHUNK_ROWS, last // CHUNK_ROWS)
        def _(chunk):
            update_chunk(chunk)
            across_copy(chunk).start()
            partner_copy(chunk).start()

    with jax.named_scope('mom0'):
        moments(GROUP_ROWS[0], GROUP_ROWS[1])
    with jax.named_scope('share0'):
        share(0)
    with jax.named_scope('mom1'):
        moments(GROUP_ROWS[1], GROUP_ROWS[2])
    with jax.named_scope('share1'):
        share(1)
    with jax.named_scope('mom2'):
        moments(GROUP_ROWS[2], EARLY_ROWS)
    with jax.named_scope('fin0'):
        finish(0)
    with jax.named_scope('mom3'):
        moments(EARLY_ROWS, GROUP_ROWS[3])
    with jax.named_scope('share2'):
        share(2)
    with jax.named_scope('fin1'):
        finish(1)
    with jax.named_scope('fin2'):
        finish(2)

    with jax.named_scope('forward'):
        @pl.loop(0, chunks)
        def _(chunk):
            across_copy(chunk).wait_recv()
            forward_copy(chunk).start()

    with jax.named_scope('tail'):
        @pl.loop(0, chunks)
        def _(chunk):
            partner_copy(chunk).wait_recv()
            forward_copy(chunk).wait_recv()

    with jax.named_scope('sends'):
        whole = new_params.at[:, pl.ds(0, width)]
        for send in (out_send.at[0], out_send.at[1], fwd_send.at[0]):
            pltpu.make_async_remote_copy(whole, whole, send, out_recv.at[0, 0], device_id=(my_model, partner), device_id_type=MESH).wait_send()
        for slot in (1, 2, 3):
            pltpu.make_async_remote_copy(gathered.at[0], gathered.at[0], sum_send.at[slot], out_recv.at[0, 0], device_id=(my_model, partner), device_id_type=MESH).wait_send()


def write_pieces(array):
    row_bytes = array.shape[1] * array.dtype.itemsize
    step = max(CHUNK_ROWS, WRITE_BYTES // row_bytes // CHUNK_ROWS * CHUNK_ROWS)
    return [(start, min(step, array.shape[0] - start)) for start in range(0, array.shape[0], step)]


def write_kernel(count, *refs):
    sources, targets, sems = refs[:count], refs[count:2 * count], refs[2 * count]
    copies = []
    for source, target in zip(sources, targets):
        for start, size in write_pieces(source):
            copies.append(pltpu.make_async_copy(source.at[pl.ds(start, size)], target.at[pl.ds(start, size)], sems.at[len(copies)]))
    for copy in copies:
        copy.start()
    for copy in copies:
        copy.wait()


def solution(mesh):
    model_size, data_size = mesh.shape['model'], mesh.shape['data']
    devices = model_size * data_size
    state_spec = P(None, ('model', 'data'))

    def device_step(local_grads, master, moment_one, moment_two):
        rows, width = master.shape
        chunks = rows // CHUNK_ROWS
        groups = len(GROUP_ROWS) - 1
        hbm = pl.BlockSpec(memory_space=pltpu.HBM)
        vmem = pl.BlockSpec(memory_space=pltpu.VMEM)
        state = pltpu.VMEM((rows, width), jnp.float32)
        held = pl.pallas_call(
            functools.partial(step_kernel, model_size, data_size),
            out_shape=(pltpu.VMEM((rows, width * data_size), jnp.bfloat16), state, state, state),
            in_specs=[hbm] * 4,
            out_specs=[vmem] * 4,
            scratch_shapes=[
                pltpu.VMEM((data_size, rows, width), jnp.bfloat16),
                pltpu.VMEM((rows, width), jnp.float32),
                pltpu.VMEM((rows, LANES), jnp.float32),
                pltpu.VMEM((rows, LANES), jnp.float32),
                pltpu.VMEM((devices, LANES), jnp.float32),
                pltpu.VMEM((1 + groups, devices, LANES), jnp.float32),
                pltpu.SemaphoreType.DMA((3,)),
                pltpu.SemaphoreType.REGULAR((LEVELS,)),
                pltpu.SemaphoreType.DMA((chunks,)),
                pltpu.SemaphoreType.DMA((data_size,)),
                pltpu.SemaphoreType.DMA((data_size, chunks)),
                pltpu.SemaphoreType.DMA((2 + groups,)),
                pltpu.SemaphoreType.DMA((2 + groups,)),
                pltpu.SemaphoreType.DMA((2,)),
                pltpu.SemaphoreType.DMA((2, chunks)),
                pltpu.SemaphoreType.DMA((1,)),
                pltpu.SemaphoreType.DMA((chunks,)),
            ],
            compiler_params=pltpu.CompilerParams(collective_id=0, has_side_effects=True, vmem_limit_bytes=38 * 2 ** 20),
            name='lamb_step',
        )(local_grads, master, moment_one, moment_two)
        return pl.pallas_call(
            functools.partial(write_kernel, len(held)),
            out_shape=tuple(jax.ShapeDtypeStruct(a.shape, a.dtype) for a in held),
            in_specs=[vmem] * len(held),
            out_specs=[hbm] * len(held),
            scratch_shapes=[pltpu.SemaphoreType.DMA((sum(len(write_pieces(a)) for a in held),))],
            compiler_params=pltpu.CompilerParams(vmem_limit_bytes=2 ** 20),
            name='write_out',
        )(*held)

    return jax.shard_map(device_step, mesh=mesh, in_specs=(P('data', None, 'model'), state_spec, state_spec, state_spec), out_specs=(P(None, 'model'), state_spec, state_spec, state_spec), check_vma=False)
```
